128 devices in a mesh: dp: 4 (over z_lo, core), seq: 8 (over x, z_hi), tensor: 4 (over y).
Axes of the slice: x: 4, y: 4, z: 4 (z_hi: 2, z_lo: 2; z = z_hi * 2 + z_lo), core: 2. Of those that a mesh axis runs over, the one named last changes fastest.
Arguments:
- latents: bfloat16 [4, 16, 256, 1152], P('dp', 'seq', 'tensor'), may hold values from -6 to 6
- modulation: float32 [4, 6, 1152], P('dp'), may hold values from -3 to 3
- in_weight: bfloat16 [1152, 3, 1152], P(None, None, 'tensor'), may hold values from -0.5 to 0.5
- out_weight: bfloat16 [1152, 1152], P('tensor'), may hold values from -0.1875 to 0.1875
- up_weight: bfloat16 [1152, 4608], P(None, 'tensor'), may hold values from -0.1875 to 0.1875
- down_weight: bfloat16 [4608, 1152], P('tensor'), may hold values from -0.09375 to 0.09375
- cotangent: bfloat16 [4, 16, 256, 1152], P('dp', 'seq', 'tensor'), may hold values from -6 to 6
Outputs:
- result: bfloat16 [4, 16, 256, 1152], P('dp', 'seq', 'tensor')
- latents_grad: bfloat16 [4, 16, 256, 1152], P('dp', 'seq', 'tensor')
- in_grad: bfloat16 [1152, 3, 1152], P(('dp', 'seq'), None, 'tensor')
- out_grad: bfloat16 [1152, 1152], P('tensor', ('dp', 'seq'))
- up_grad: bfloat16 [1152, 4608], P(('dp', 'seq'), 'tensor')
- down_grad: bfloat16 [4608, 1152], P('tensor', ('dp', 'seq'))
The draws below stay inside these ranges and needn't reach their ends.
All inputs are finite; a program needn't handle non-finite values.
Results may differ from the reference program's by a relative error of at most 0.02.
The reference program's roundings to bfloat16 on the way count: a program that leaves them out, or rounds other values in their place, can miss the bound.
Values may be sent and summed in bfloat16 or wider, within the bound.
No kernel may reach another device: no remote copies, remote signals or barrier semaphores. Data moves between devices by JAX's collectives and lax.ppermute only.
A program may use at most 128 MiB of HBM per device.

```python
import math
import jax
import jax.numpy as jnp
from jax import lax

D = 1152
HEADS = 16
FF = 4608
PIX = 256
FRAMES = 16
BATCH = 4


def draw_latents(key, part):
    shape = (BATCH, FRAMES, PIX, D)
    values = jax.random.normal(key, shape, jnp.float32)
    return jnp.clip(values, -6.0, 6.0).astype(jnp.bfloat16)


def draw_in_weight(key, part):
    first_key = jax.random.fold_in(key, 0)
    basis = jax.random.normal(first_key, (D, 3, D), jnp.float32) * D ** (-0.5)
    values = basis
    return jnp.clip(values, -0.5, 0.5).astype(jnp.bfloat16)


def with_spikes(values, rng, source, target, shards_of, factor):
    def block_of(position):
        return (jnp.arange(values.shape[position]) // (values.shape[position] // shards_of)).reshape((-1,) + (1,) * (values.ndim - 1 - position))

    one_side = jax.random.permutation(rng, shards_of)[block_of(target)]
    far = (block_of(target) + shards_of // 2) % shards_of
    return jnp.where((block_of(source) == one_side) | (block_of(source) == far), factor * values, values)


def level_of(stream_key, shape, cuts, least, largest):
    gain = 1.0
    for axis_at, blocks in cuts:
        draws = jax.random.uniform(jax.random.fold_in(jax.random.fold_in(stream_key, 6), axis_at), (blocks,), jnp.float32, least / len(cuts), largest / len(cuts))
        gain = gain * jnp.repeat(jnp.exp(draws), shape[axis_at] // blocks).reshape((-1,) + (1,) * (len(shape) - 1 - axis_at))
    return gain


def gaussian(own_key, extent, scale, reach, cuts=(), kind=jnp.bfloat16):
    values = scale * jax.random.normal(own_key, extent, jnp.float32)
    if cuts:
        values = values * level_of(own_key, extent, cuts, -0.22, 0.18)
    return jnp.clip(values, -reach, reach).astype(kind)


def gaussian_with(rng, extent, scale, limit, cuts, heavy, dtype=jnp.bfloat16):
    entries = scale * jax.random.normal(rng, extent, jnp.float32)
    if cuts:
        entries = entries * level_of(rng, extent, cuts, -0.22, 0.18)
    return jnp.clip(with_spikes(entries, jax.random.fold_in(rng, 3), *heavy), -limit, limit).astype(dtype)


def setup_inputs(seed: int = 0) -> dict:
    keys = jax.random.split(jax.random.key(seed), 8)
    latents = draw_latents(jax.random.fold_in(keys[7], 71), 0)
    modulation = gaussian(keys[1], (BATCH, 6, D), 0.5, 3.0, ((0, 4),), jnp.float32)
    in_weight = draw_in_weight(jax.random.fold_in(keys[7], 71), 0)
    out_weight = gaussian(keys[3], (D, D), D ** -0.5, 0.1875, ((0, 4),))
    up_weight = gaussian(keys[4], (D, FF), D ** -0.5, 0.1875, ((1, 4),))
    down_weight = gaussian(keys[5], (FF, D), FF ** -0.5, 0.09375, ((0, 4),))
    cotangent = gaussian_with(keys[6], (BATCH, FRAMES, PIX, D), 1.0, 6.0, ((0, 4), (1, 8), (2, 4)), (1, 3, 8, 2.0))
    return {"latents": latents, "modulation": modulation, "in_weight": in_weight, "out_weight": out_weight, "up_weight": up_weight, "down_weight": down_weight, "cotangent": cotangent}


epsilon = 1e-06

def normalize(rows):
    center = lax.optimization_barrier(jnp.mean(rows, axis=-1, keepdims=True))
    centred = rows - center
    spread = lax.optimization_barrier(jnp.mean(centred * centred, axis=-1, keepdims=True))
    inverse = lax.rsqrt(spread + epsilon)
    return (centred * inverse, inverse)

def norm_back(normed, inverse, upstream):
    mean_grad = lax.optimization_barrier(jnp.mean(upstream, axis=-1, keepdims=True))
    mean_cross = lax.optimization_barrier(jnp.mean(upstream * normed, axis=-1, keepdims=True))
    return (upstream - mean_grad - normed * mean_cross) * inverse

def gelu_tanh(values):
    return jax.nn.gelu(values, approximate=True)

def flat_dot(left, right):
    leading = left.shape[:-1]
    out_rows = jnp.dot(left.reshape(-1, left.shape[-1]), right, preferred_element_type=jnp.float32)
    return out_rows.reshape(leading + (right.shape[-1],))

def flat_dot_t(left, right):
    leading = left.shape[:-1]
    out_rows = lax.dot_general(left.reshape(-1, left.shape[-1]), right, (((1,), (1,)), ((), ())), preferred_element_type=jnp.float32)
    return out_rows.reshape(leading + (right.shape[0],))

def weight_grad(left, right):
    return lax.dot_general(left.reshape(-1, left.shape[-1]), right.reshape(-1, right.shape[-1]), (((0,), (0,)), ((), ())), preferred_element_type=jnp.float32)

def attend(queries, key_rows, value_rows):
    scaling = 1.0 / math.sqrt(queries.shape[-1])
    scores = jnp.einsum('bfphe,bgphe->bphfg', queries.astype(jnp.float32), key_rows.astype(jnp.float32)) * scaling
    highest = lax.optimization_barrier(jnp.max(scores, axis=-1, keepdims=True))
    raised = jnp.exp(scores - highest)
    probs = raised / lax.optimization_barrier(jnp.sum(raised, axis=-1, keepdims=True))
    probs_low = probs.astype(jnp.bfloat16)
    attended = jnp.einsum('bphfg,bgphe->bfphe', probs_low.astype(jnp.float32), value_rows.astype(jnp.float32)).astype(jnp.bfloat16)
    return (attended, probs, probs_low)

def attend_back(queries, key_rows, value_rows, probs, probs_low, attended_grad):
    scaling = 1.0 / math.sqrt(queries.shape[-1])
    grad_wide = attended_grad.astype(jnp.float32)
    value_grad = jnp.einsum('bphfg,bfphe->bgphe', probs_low.astype(jnp.float32), grad_wide).astype(jnp.bfloat16)
    prob_grad = jnp.einsum('bfphe,bgphe->bphfg', grad_wide, value_rows.astype(jnp.float32))
    score_grad = probs * (prob_grad - lax.optimization_barrier(jnp.sum(probs * prob_grad, axis=-1, keepdims=True))) * scaling
    score_low = score_grad.astype(jnp.bfloat16).astype(jnp.float32)
    query_grad = jnp.einsum('bphfg,bgphe->bfphe', score_low, key_rows.astype(jnp.float32)).astype(jnp.bfloat16)
    key_grad = jnp.einsum('bphfg,bfphe->bgphe', score_low, queries.astype(jnp.float32)).astype(jnp.bfloat16)
    return (query_grad, key_grad, value_grad)

def reference(latents, modulation, in_weight, out_weight, up_weight, down_weight, cotangent):
    samples, frames_all, patches, width = latents.shape
    modulate = modulation[:, :, None, None, :]
    shift_first, scale_first, gate_first = (modulate[:, 0], modulate[:, 1], modulate[:, 2])
    shift_second, scale_second, gate_second = (modulate[:, 3], modulate[:, 4], modulate[:, 5])
    inputs = latents.astype(jnp.float32)
    first_normed, first_inverse = normalize(inputs)
    first_input = (first_normed * (1.0 + scale_first) + shift_first).astype(jnp.bfloat16)
    in_flat = in_weight.reshape(width, 3 * width)
    projected = flat_dot(first_input, in_flat).astype(jnp.bfloat16)
    split_parts = projected.reshape(samples, frames_all, patches, 3, HEADS, width // HEADS)
    queries, key_rows, value_rows = (split_parts[:, :, :, 0], split_parts[:, :, :, 1], split_parts[:, :, :, 2])
    attended, probs, probs_low = attend(queries, key_rows, value_rows)
    attended_flat = attended.reshape(samples, frames_all, patches, width)
    midway = inputs + gate_first * flat_dot(attended_flat, out_weight)
    second_normed, second_inverse = normalize(midway)
    second_input = (second_normed * (1.0 + scale_second) + shift_second).astype(jnp.bfloat16)
    hidden = flat_dot(second_input, up_weight)
    activated = gelu_tanh(hidden).astype(jnp.bfloat16)
    result = (midway + gate_second * flat_dot(activated, down_weight)).astype(jnp.bfloat16)
    upstream = cotangent.astype(jnp.float32)
    branch_grad = (gate_second * upstream).astype(jnp.bfloat16)
    down_grad = weight_grad(activated, branch_grad)
    activated_grad = flat_dot_t(branch_grad, down_weight)
    hidden_grad = jax.vjp(gelu_tanh, hidden)[1](activated_grad)[0].astype(jnp.bfloat16)
    up_grad = weight_grad(second_input, hidden_grad)
    second_grad = flat_dot_t(hidden_grad, up_weight)
    midway_grad = upstream + norm_back(second_normed, second_inverse, second_grad * (1.0 + scale_second))
    attention_grad = (gate_first * midway_grad).astype(jnp.bfloat16)
    out_grad = weight_grad(attended_flat, attention_grad)
    attended_grad = flat_dot_t(attention_grad, out_weight).astype(jnp.bfloat16)
    attended_grad = attended_grad.reshape(samples, frames_all, patches, HEADS, width // HEADS)
    query_grad, key_grad, value_grad = attend_back(queries, key_rows, value_rows, probs, probs_low, attended_grad)
    projected_grad = jnp.stack([query_grad, key_grad, value_grad], axis=3).reshape(samples, frames_all, patches, 3 * width)
    in_grad = weight_grad(first_input, projected_grad).reshape(width, 3, width)
    first_grad = flat_dot_t(projected_grad, in_flat)
    latents_grad = (midway_grad + norm_back(first_normed, first_inverse, first_grad * (1.0 + scale_first))).astype(jnp.bfloat16)
    return (result, latents_grad, in_grad.astype(jnp.bfloat16), out_grad.astype(jnp.bfloat16), up_grad.astype(jnp.bfloat16), down_grad.astype(jnp.bfloat16))
```

```python
import functools
import math

import jax
import jax.numpy as jnp
from jax import lax
from jax.experimental import pallas as pl
from jax.experimental.pallas import tpu as pltpu
from jax.sharding import PartitionSpec as P

HEAD_DIM = 72
EPS = 1e-06
F32 = jnp.float32
BF16 = jnp.bfloat16


def dot(a, b, da=1, db=0):
    return lax.dot_general(a, b, (((da,), (db,)), ((), ())), preferred_element_type=F32)


def call(kernel, outs, *args, flops=0, scratch=(), name=None):
    return pl.pallas_call(
        kernel,
        out_shape=[jax.ShapeDtypeStruct(s, d) for s, d in outs],
        scratch_shapes=list(scratch),
        cost_estimate=pl.CostEstimate(flops=int(flops), transcendentals=0, bytes_accessed=0),
        name=name,
    )(*args)


def normalize(rows):
    center = jnp.mean(rows, axis=-1, keepdims=True)
    centred = rows - center
    spread = jnp.mean(centred * centred, axis=-1, keepdims=True)
    inverse = lax.rsqrt(spread + EPS)
    return centred * inverse, inverse


def norm_back(normed, inverse, upstream):
    mean_grad = jnp.mean(upstream, axis=-1, keepdims=True)
    mean_cross = jnp.mean(upstream * normed, axis=-1, keepdims=True)
    return (upstream - mean_grad - normed * mean_cross) * inverse


def total(refs):
    out = refs[0][...].astype(F32)
    for r in refs[1:]:
        out = out + r[...].astype(F32)
    return out


def first_kernel(x_ref, mod_ref, out_ref):
    normed, _ = normalize(x_ref[...].astype(F32))
    out_ref[...] = (normed * (1.0 + mod_ref[1:2, :]) + mod_ref[0:1, :]).astype(BF16)


def branch_kernel(c_ref, mod_ref, out_ref):
    out_ref[...] = (mod_ref[5:6, :] * c_ref[...].astype(F32)).astype(BF16)


def midway_kernel(x_ref, mod_ref, *refs):
    *parts, mid_ref, out_ref = refs
    mid = x_ref[...].astype(F32) + mod_ref[2:3, :] * total(parts)
    mid_ref[...] = mid
    normed, _ = normalize(mid)
    out_ref[...] = (normed * (1.0 + mod_ref[4:5, :]) + mod_ref[3:4, :]).astype(BF16)


def result_kernel(mid_ref, mod_ref, *refs):
    *parts, out_ref = refs
    out_ref[...] = (mid_ref[...] + mod_ref[5:6, :] * total(parts)).astype(BF16)


def midgrad_kernel(c_ref, mid_ref, mod_ref, *refs):
    *parts, grad_ref, out_ref = refs
    normed, inverse = normalize(mid_ref[...])
    up = total(parts) * (1.0 + mod_ref[4:5, :])
    grad = c_ref[...].astype(F32) + norm_back(normed, inverse, up)
    grad_ref[...] = grad
    out_ref[...] = (mod_ref[2:3, :] * grad).astype(BF16)


def last_kernel(x_ref, grad_ref, mod_ref, *refs):
    *parts, out_ref = refs
    normed, inverse = normalize(x_ref[...].astype(F32))
    up = total(parts) * (1.0 + mod_ref[1:2, :])
    out_ref[...] = (grad_ref[...] + norm_back(normed, inverse, up)).astype(BF16)


def head_masks(width, dtype):
    lane = lax.broadcasted_iota(jnp.int32, (1, width), 1)
    masks = []
    for h in range(width // HEAD_DIM):
        inside = jnp.logical_and(lane >= h * HEAD_DIM, lane < (h + 1) * HEAD_DIM)
        masks.append(jnp.where(inside, 1.0, 0.0).astype(dtype))
    return masks


def softmax_of(stacked_q, key_rows, block):
    scaling = 1.0 / math.sqrt(HEAD_DIM)
    scores = dot(stacked_q, key_rows, 1, 1) * scaling
    row = lax.broadcasted_iota(jnp.int32, scores.shape, 0)
    col = lax.broadcasted_iota(jnp.int32, scores.shape, 1)
    same = (row & (block - 1)) == (col & (block - 1))
    scores = jnp.where(same, scores, -1e30)
    raised = jnp.exp(scores - jnp.max(scores, axis=-1, keepdims=True))
    return raised / jnp.sum(raised, axis=-1, keepdims=True)


def attend_kernel(x_ref, wi_ref, wo_ref, proj_ref, att_ref, part_ref, *, block):
    n = x_ref.shape[0]
    width = wo_ref.shape[0]
    proj = dot(x_ref[...], wi_ref[...]).astype(BF16)
    proj_ref[...] = proj
    q, k, v = (proj[:, j * width : (j + 1) * width] for j in range(3))
    masks = head_masks(width, BF16)
    probs = softmax_of(jnp.concatenate([q * m for m in masks], axis=0), k, block)
    mixed = dot(probs.astype(BF16), v)
    att = sum(mixed[h * n : (h + 1) * n] * m for h, m in enumerate(head_masks(width, F32)))
    att = att.astype(BF16)
    att_ref[...] = att
    part_ref[...] = dot(att, wo_ref[...]).astype(BF16)


def attend_back_kernel(g_ref, proj_ref, wi_ref, wo_ref, dproj_ref, part_ref, *, block):
    n = g_ref.shape[0]
    width = wo_ref.shape[0]
    scaling = 1.0 / math.sqrt(HEAD_DIM)
    att_grad = dot(g_ref[...], wo_ref[...], 1, 1).astype(BF16)
    proj = proj_ref[...]
    q, k, v = (proj[:, j * width : (j + 1) * width] for j in range(3))
    masks = head_masks(width, BF16)
    stacked_q = jnp.concatenate([q * m for m in masks], axis=0)
    stacked_g = jnp.concatenate([att_grad * m for m in masks], axis=0)
    probs = softmax_of(stacked_q, k, block)
    prob_grad = dot(stacked_g, v, 1, 1)
    inner = jnp.sum(probs * prob_grad, axis=-1, keepdims=True)
    score_low = (probs * (prob_grad - inner) * scaling).astype(BF16)
    mixed = dot(score_low, k)
    dq = sum(mixed[h * n : (h + 1) * n] * m for h, m in enumerate(head_masks(width, F32)))
    dk = dot(score_low, stacked_q, 0, 0)
    dv = dot(probs.astype(BF16), stacked_g, 0, 0)
    dproj = jnp.concatenate([dq, dk, dv], axis=1).astype(BF16)
    dproj_ref[...] = dproj
    part_ref[...] = dot(dproj, wi_ref[...], 1, 1).astype(BF16)


def mlp_kernel(x_ref, b_ref, up_ref, down_ref, act_ref, hg_ref, part_ref):
    cube = 0.044715
    root = math.sqrt(2.0 / math.pi)
    act_grad = dot(b_ref[...], down_ref[...], 1, 1)
    v = dot(x_ref[...], up_ref[...])
    squared = v * v
    t = jnp.tanh(root * (v + cube * squared * v))
    half = 0.5 * (1.0 + t)
    act_ref[...] = (v * half).astype(BF16)
    slope = half + 0.5 * v * (1.0 - t * t) * (root * (1.0 + 3.0 * cube * squared))
    hg = (act_grad * slope).astype(BF16)
    hg_ref[...] = hg
    part_ref[...] = dot(hg, up_ref[...], 1, 1).astype(BF16)


def product_kernel(a_ref, b_ref, out_ref):
    out_ref[...] = dot(a_ref[...], b_ref[...]).astype(BF16)


def grads_kernel(*refs, pieces, sets, order, rows):
    ins, out_ref, acc_ref = refs[:-2], refs[-2], refs[-1]
    at = 0
    depth = ins[0].shape[1]
    tall = out_ref.shape[1]
    for s in range(sets):
        left = jnp.concatenate([r[...] for r in ins[2 * s * pieces : (2 * s + 1) * pieces]], axis=0)
        rights = ins[(2 * s + 1) * pieces : (2 * s + 2) * pieces]
        right = jnp.concatenate([r[...] for r in rights], axis=0)
        width = right.shape[1]
        acc_ref[0:depth, 0:width] = dot(left, right, 0, 0)
        acc_ref[depth:, 0:width] = jnp.zeros((acc_ref.shape[0] - depth, width), F32)
        for g, to in enumerate(order):
            out_ref[to, :, at : at + width] = acc_ref[g * rows : g * rows + tall, 0:width].astype(BF16)
        at += width


def weight_grads(sets, order):
    pieces = len(sets[0][0])
    depth = sets[0][0][0].shape[1]
    rows = depth // len(order)
    tall = -(-rows // 8) * 8
    widths = [right[0].shape[1] for _, right in sets]
    flat = [a for left, right in sets for a in (*left, *right)]
    n = sum(p.shape[0] for p in sets[0][0])
    return call(
        functools.partial(grads_kernel, pieces=pieces, sets=len(sets), order=order, rows=rows),
        [((len(order), tall, sum(widths)), BF16)],
        *flat,
        flops=2 * n * depth * sum(widths),
        scratch=[pltpu.VMEM((depth + 8, max(widths)), F32)],
        name="weight_grads",
    )[0]


def shift(x, axis, k):
    size = lax.axis_size(axis)
    return lax.ppermute(x, axis, [(i, (i + k) % size) for i in range(size)])


def gathered(x):
    return [x] + [shift(x, "tensor", k) for k in range(1, lax.axis_size("tensor"))]


def returned(parts):
    return [parts[0]] + [shift(p, "tensor", -k) for k, p in enumerate(parts) if k]


class Torus:
    def __init__(self):
        self.dp, self.seq = lax.axis_size("dp"), lax.axis_size("seq")
        self.cores, self.zlo, self.zhi = 2, self.dp // 2, 2
        self.xs, self.zs = self.seq // 2, 2 * (self.dp // 2)

    def linear(self, core, x, z):
        zh, zl = z // self.zlo, z % self.zlo
        return (zl * self.cores + core) * self.seq + x * self.zhi + zh

    def spots(self):
        return [(c, x, z) for c in range(self.cores) for x in range(self.xs) for z in range(self.zs)]

    def here(self):
        dp, seq = lax.axis_index("dp"), lax.axis_index("seq")
        return dp % 2, seq // 2, (seq % 2) * self.zlo + dp // 2

    def order(self):
        to = [0] * (self.dp * self.seq)
        for at, spot in enumerate(self.spots()):
            to[self.linear(*spot)] = at
        return tuple(to)

    def shift(self, array, which, k):
        sizes = (self.cores, self.xs, self.zs)
        pairs = []
        for spot in self.spots():
            there = list(spot)
            there[which] = (there[which] + k) % sizes[which]
            pairs.append((self.linear(*spot), self.linear(*there)))
        return lax.ppermute(array, ("dp", "seq"), pairs)

    def scatter_sum(self, chunks):
        sizes = (self.cores, self.xs, self.zs)
        value = chunks.reshape(*sizes, *chunks.shape[1:])
        for which, here in enumerate(self.here()):
            size = sizes[which]
            kept = lax.dynamic_index_in_dim(value, here, 0, keepdims=False).astype(F32)
            arrived = [
                self.shift(
                    lax.dynamic_index_in_dim(value, (here + k) % size, 0, keepdims=False), which, k
                )
                for k in range(1, size)
            ]
            for a in arrived:
                kept = kept + a.astype(F32)
            value = kept.astype(BF16)
        return value


def to_pixels(x):
    _, frames, pixels, width = x.shape
    size = lax.axis_size("seq")
    cut = x.reshape(frames, size, pixels // size, width).transpose(1, 0, 2, 3)
    cut = cut.reshape(size, -1, width)
    return lax.all_to_all(cut, "seq", 0, 0, tiled=True).reshape(-1, width)


def to_frames(x, shape):
    _, frames, pixels, width = shape
    size = lax.axis_size("seq")
    back = lax.all_to_all(x.reshape(size, -1, width), "seq", 0, 0, tiled=True)
    back = back.reshape(size, frames, pixels // size, width).transpose(1, 0, 2, 3)
    return back.reshape(shape)


def body(latents, modulation, in_weight, out_weight, up_weight, down_weight, cotangent):
    width = latents.shape[-1]
    local = out_weight.shape[0]
    units = up_weight.shape[1]
    block = latents.shape[2] // lax.axis_size("seq")
    mod = modulation[0]
    wi = in_weight.reshape(width, 3 * local)
    tokens = to_pixels(latents)
    upstream = to_pixels(cotangent)
    n = tokens.shape[0]
    low = ((n, width), BF16)
    wide = ((n, width), F32)

    first_input = call(first_kernel, [low], tokens, mod, flops=20 * n * width, name="first")[0]
    first_full = gathered(first_input)
    branch = call(branch_kernel, [low], upstream, mod, flops=4 * n * width, name="branch")[0]
    branch_full = gathered(branch)

    heads = local // HEAD_DIM
    attn_flops = 2 * n * width * 4 * local + 4 * heads * n * n * local
    projected, attended, parts = [], [], []
    for piece in first_full:
        proj, att, part = call(
            functools.partial(attend_kernel, block=block),
            [((n, 3 * local), BF16), ((n, local), BF16), low],
            piece, wi, out_weight, flops=attn_flops, name="attend",
        )
        projected.append(proj)
        attended.append(att)
        parts.append(part)
    midway, second_input = call(
        midway_kernel, [wide, low], tokens, mod, *returned(parts), flops=20 * n * width, name="midway"
    )
    second_full = gathered(second_input)
    activated, hidden_grad, parts = [], [], []
    for piece, b in zip(second_full, branch_full):
        act, hg, part = call(
            mlp_kernel,
            [((n, units), BF16), ((n, units), BF16), low],
            piece, b, up_weight, down_weight, flops=6 * n * width * units, name="mlp",
        )
        activated.append(act)
        hidden_grad.append(hg)
        parts.append(part)
    midway_grad, attention_grad = call(
        midgrad_kernel, [wide, low], upstream, midway, mod, *returned(parts),
        flops=30 * n * width, name="midgrad",
    )
    torus = Torus()
    dp_size, seq_size = lax.axis_size("dp"), lax.axis_size("seq")
    offload_order = tuple((g % seq_size) * dp_size + g // seq_size for g in range(dp_size * seq_size))
    mlp_chunks = weight_grads([(branch_full, activated), (second_full, hidden_grad)], offload_order)
    mlp_sum = lax.psum_scatter(mlp_chunks, ("seq", "dp"), scatter_dimension=0, tiled=False)

    attention_full = gathered(attention_grad)
    projected_grad, parts = [], []
    for piece, proj in zip(attention_full, projected):
        dproj, part = call(
            functools.partial(attend_back_kernel, block=block),
            [((n, 3 * local), BF16), low],
            piece, proj, wi, out_weight, flops=2 * attn_flops, name="attend_back",
        )
        projected_grad.append(dproj)
        parts.append(part)
    latents_grad = call(
        last_kernel, [low], tokens, midway_grad, mod, *returned(parts), flops=30 * n * width, name="last"
    )[0]

    ff = [
        call(product_kernel, [low], a, down_weight, flops=2 * n * width * units, name="ff")[0]
        for a in activated
    ]
    result = call(result_kernel, [low], midway, mod, *returned(ff), flops=10 * n * width, name="result")[0]

    attn_chunks = weight_grads(
        [(first_full, projected_grad), (attention_full, attended)], torus.order()
    )
    attn_sum = torus.scatter_sum(attn_chunks)
    rows = width // (dp_size * seq_size)
    in_grad = attn_sum[:rows, : 3 * local].reshape(rows, 3, local)
    out_grad = attn_sum[:rows, 3 * local :].T
    down_grad = mlp_sum[:rows, :units].T
    up_grad = mlp_sum[:rows, units:]
    return (
        to_frames(result, latents.shape),
        to_frames(latents_grad, latents.shape),
        in_grad,
        out_grad,
        up_grad,
        down_grad,
    )


def solution(mesh):
    placed = (
        P("dp", "seq", "tensor", None),
        P("dp", None, None),
        P(None, None, "tensor"),
        P("tensor", None),
        P(None, "tensor"),
        P("tensor", None),
        P("dp", "seq", "tensor", None),
    )
    return jax.shard_map(
        body,
        mesh=mesh,
        in_specs=placed,
        out_specs=(
            P("dp", "seq", "tensor", None),
            P("dp", "seq", "tensor", None),
            P(("dp", "seq"), None, "tensor"),
            P("tensor", ("dp", "seq")),
            P(("dp", "seq"), "tensor"),
            P("tensor", ("dp", "seq")),
        ),
        check_vma=False,
    )
```

```python
import functools
import math

import jax
import jax.numpy as jnp
from jax import lax
from jax.experimental import pallas as pl
from jax.experimental.pallas import tpu as pltpu
from jax.sharding import PartitionSpec as P


HEAD_DIM = 72
EPS = 1e-06
F32 = jnp.float32
BF16 = jnp.bfloat16


def dot(a, b, da=1, db=0):
    return lax.dot_general(a, b, (((da,), (db,)), ((), ())), preferred_element_type=F32)


def call(kernel, outs, *args, flops=0, scratch=(), room=16):
    return pl.pallas_call(
        kernel,
        out_shape=[jax.ShapeDtypeStruct(s, d) for s, d in outs],
        scratch_shapes=list(scratch),
        cost_estimate=pl.CostEstimate(flops=int(flops), transcendentals=0, bytes_accessed=0),
        compiler_params=pltpu.CompilerParams(vmem_limit_bytes=room << 20),
    )(*args)


def normalize(rows):
    center = jnp.mean(rows, axis=-1, keepdims=True)
    centred = rows - center
    spread = jnp.mean(centred * centred, axis=-1, keepdims=True)
    inverse = lax.rsqrt(spread + EPS)
    return centred * inverse, inverse


def norm_back(normed, inverse, upstream):
    mean_grad = jnp.mean(upstream, axis=-1, keepdims=True)
    mean_cross = jnp.mean(upstream * normed, axis=-1, keepdims=True)
    return (upstream - mean_grad - normed * mean_cross) * inverse


def total(refs):
    out = refs[0][...].astype(F32)
    for r in refs[1:]:
        out = out + r[...].astype(F32)
    return out


def first_kernel(x_ref, mod_ref, out_ref):
    normed, _ = normalize(x_ref[...].astype(F32))
    out_ref[...] = (normed * (1.0 + mod_ref[1:2, :]) + mod_ref[0:1, :]).astype(BF16)


def branch_kernel(c_ref, mod_ref, out_ref):
    out_ref[...] = (mod_ref[5:6, :] * c_ref[...].astype(F32)).astype(BF16)


def midway_kernel(x_ref, mod_ref, *refs):
    *parts, mid_ref, out_ref = refs
    mid = x_ref[...].astype(F32) + mod_ref[2:3, :] * total(parts)
    mid_ref[...] = mid
    normed, _ = normalize(mid)
    out_ref[...] = (normed * (1.0 + mod_ref[4:5, :]) + mod_ref[3:4, :]).astype(BF16)


def result_kernel(mid_ref, mod_ref, *refs):
    *parts, out_ref = refs
    out_ref[...] = (mid_ref[...] + mod_ref[5:6, :] * total(parts)).astype(BF16)


def midgrad_kernel(c_ref, mid_ref, mod_ref, *refs):
    *parts, grad_ref, out_ref = refs
    normed, inverse = normalize(mid_ref[...])
    up = total(parts) * (1.0 + mod_ref[4:5, :])
    grad = c_ref[...].astype(F32) + norm_back(normed, inverse, up)
    grad_ref[...] = grad
    out_ref[...] = (mod_ref[2:3, :] * grad).astype(BF16)


def last_kernel(x_ref, grad_ref, mod_ref, *refs):
    *parts, out_ref = refs
    normed, inverse = normalize(x_ref[...].astype(F32))
    up = total(parts) * (1.0 + mod_ref[1:2, :])
    out_ref[...] = (grad_ref[...] + norm_back(normed, inverse, up)).astype(BF16)


def head_masks(width, dtype):
    lane = lax.broadcasted_iota(jnp.int32, (1, width), 1)
    masks = []
    for h in range(width // HEAD_DIM):
        inside = jnp.logical_and(lane >= h * HEAD_DIM, lane < (h + 1) * HEAD_DIM)
        masks.append(jnp.where(inside, 1.0, 0.0).astype(dtype))
    return masks


def softmax_of(stacked_q, key_rows, block):
    scaling = 1.0 / math.sqrt(HEAD_DIM)
    scores = dot(stacked_q, key_rows, 1, 1) * scaling
    row = lax.broadcasted_iota(jnp.int32, scores.shape, 0)
    col = lax.broadcasted_iota(jnp.int32, scores.shape, 1)
    same = (row & (block - 1)) == (col & (block - 1))
    scores = jnp.where(same, scores, -1e30)
    raised = jnp.exp(scores - jnp.max(scores, axis=-1, keepdims=True))
    return raised / jnp.sum(raised, axis=-1, keepdims=True)


def attend_kernel(x_ref, wi_ref, wo_ref, proj_ref, att_ref, part_ref, *, block):
    n = x_ref.shape[0]
    width = wo_ref.shape[0]
    proj = dot(x_ref[...], wi_ref[...]).astype(BF16)
    proj_ref[...] = proj
    q, k, v = (proj[:, j * width : (j + 1) * width] for j in range(3))
    masks = head_masks(width, BF16)
    probs = softmax_of(jnp.concatenate([q * m for m in masks], axis=0), k, block)
    mixed = dot(probs.astype(BF16), v)
    att = sum(mixed[h * n : (h + 1) * n] * m for h, m in enumerate(head_masks(width, F32)))
    att = att.astype(BF16)
    att_ref[...] = att
    part_ref[...] = dot(att, wo_ref[...]).astype(BF16)


def attend_back_kernel(g_ref, proj_ref, wi_ref, wo_ref, dproj_ref, part_ref, *, block):
    n = g_ref.shape[0]
    width = wo_ref.shape[0]
    scaling = 1.0 / math.sqrt(HEAD_DIM)
    att_grad = dot(g_ref[...], wo_ref[...], 1, 1).astype(BF16)
    proj = proj_ref[...]
    q, k, v = (proj[:, j * width : (j + 1) * width] for j in range(3))
    masks = head_masks(width, BF16)
    stacked_q = jnp.concatenate([q * m for m in masks], axis=0)
    stacked_g = jnp.concatenate([att_grad * m for m in masks], axis=0)
    probs = softmax_of(stacked_q, k, block)
    prob_grad = dot(stacked_g, v, 1, 1)
    inner = jnp.sum(probs * prob_grad, axis=-1, keepdims=True)
    score_low = (probs * (prob_grad - inner) * scaling).astype(BF16)
    mixed = dot(score_low, k)
    dq = sum(mixed[h * n : (h + 1) * n] * m for h, m in enumerate(head_masks(width, F32)))
    dk = dot(score_low, stacked_q, 0, 0)
    dv = dot(probs.astype(BF16), stacked_g, 0, 0)
    dproj = jnp.concatenate([dq, dk, dv], axis=1).astype(BF16)
    dproj_ref[...] = dproj
    part_ref[...] = dot(dproj, wi_ref[...], 1, 1).astype(BF16)


def mlp_kernel(x_ref, b_ref, up_ref, down_ref, act_ref, hg_ref, part_ref):
    cube = 0.044715
    root = math.sqrt(2.0 / math.pi)
    act_grad = dot(b_ref[...], down_ref[...], 1, 1)
    v = dot(x_ref[...], up_ref[...])
    squared = v * v
    t = jnp.tanh(root * (v + cube * squared * v))
    half = 0.5 * (1.0 + t)
    act_ref[...] = (v * half).astype(BF16)
    slope = half + 0.5 * v * (1.0 - t * t) * (root * (1.0 + 3.0 * cube * squared))
    hg = (act_grad * slope).astype(BF16)
    hg_ref[...] = hg
    part_ref[...] = dot(hg, up_ref[...], 1, 1).astype(BF16)


def product_kernel(a_ref, b_ref, out_ref):
    out_ref[...] = dot(a_ref[...], b_ref[...]).astype(BF16)


def grads_kernel(*refs, pieces, sets, order, rows):
    ins, out_ref, acc_ref = refs[:-2], refs[-2], refs[-1]
    at = 0
    depth = ins[0].shape[1]
    tall = out_ref.shape[1]
    for s in range(sets):
        left = jnp.concatenate([r[...] for r in ins[2 * s * pieces : (2 * s + 1) * pieces]], axis=0)
        rights = ins[(2 * s + 1) * pieces : (2 * s + 2) * pieces]
        right = jnp.concatenate([r[...] for r in rights], axis=0)
        width = right.shape[1]
        acc_ref[0:depth, 0:width] = dot(left, right, 0, 0)
        acc_ref[depth:, 0:width] = jnp.zeros((acc_ref.shape[0] - depth, width), F32)
        for g, to in enumerate(order):
            out_ref[to, :, at : at + width] = acc_ref[g * rows : g * rows + tall, 0:width].astype(BF16)
        at += width


def weight_grads(sets, order):
    pieces = len(sets[0][0])
    depth = sets[0][0][0].shape[1]
    rows = depth // len(order)
    tall = -(-rows // 8) * 8
    widths = [right[0].shape[1] for _, right in sets]
    flat = [a for left, right in sets for a in (*left, *right)]
    n = sum(p.shape[0] for p in sets[0][0])
    return call(
        functools.partial(grads_kernel, pieces=pieces, sets=len(sets), order=order, rows=rows),
        [((len(order), tall, sum(widths)), BF16)],
        *flat,
        flops=2 * n * depth * sum(widths),
        scratch=[pltpu.VMEM((depth + 8, max(widths)), F32)],
        room=36,
    )[0]


def shift(x, axis, k):
    size = lax.axis_size(axis)
    return lax.ppermute(x, axis, [(i, (i + k) % size) for i in range(size)])


def gathered(x):
    return [x] + [shift(x, "tensor", k) for k in range(1, lax.axis_size("tensor"))]


def returned(parts):
    return [parts[0]] + [shift(p, "tensor", -k) for k, p in enumerate(parts) if k]


def pick(array, at):
    start = (at,) + (jnp.uint32(0),) * (array.ndim - 1)
    return lax.dynamic_slice(array, start, (1, *array.shape[1:])).reshape(array.shape[1:])


class Torus:
    def __init__(self):
        self.dp, self.seq = lax.axis_size("dp"), lax.axis_size("seq")
        self.zlo, self.zhi = self.dp // 2, 2
        self.sizes = (2, self.seq // 2, self.zlo * 2)

    def linear(self, core, x, z):
        zh, zl = z // self.zlo, z % self.zlo
        return (zl * 2 + core) * self.seq + x * self.zhi + zh

    def spots(self):
        cores, xs, zs = self.sizes
        return [(c, x, z) for c in range(cores) for x in range(xs) for z in range(zs)]

    def here(self):
        dp, seq = (lax.axis_index(a).astype(jnp.uint32) for a in ("dp", "seq"))
        two = jnp.uint32(2)
        return (
            lax.rem(dp, two),
            lax.div(seq, two),
            lax.rem(seq, two) * jnp.uint32(self.zlo) + lax.div(dp, two),
        )

    def order(self):
        to = [0] * (self.dp * self.seq)
        for at, spot in enumerate(self.spots()):
            to[self.linear(*spot)] = at
        return tuple(to)

    def shift(self, array, which, k):
        pairs = []
        for spot in self.spots():
            there = list(spot)
            there[which] = (there[which] + k) % self.sizes[which]
            pairs.append((self.linear(*spot), self.linear(*there)))
        return lax.ppermute(array, ("dp", "seq"), pairs)

    def scatter_sum(self, chunks):
        value = chunks.reshape(*self.sizes, *chunks.shape[1:])
        for which, here in enumerate(self.here()):
            size = self.sizes[which]
            kept = pick(value, here).astype(F32)
            for k in range(1, size):
                part = pick(value, lax.rem(here + jnp.uint32(k), jnp.uint32(size)))
                arrived = self.shift(part, which, k)
                kept = kept + arrived.astype(F32)
            value = kept.astype(BF16)
        return value


def to_pixels(x):
    _, frames, pixels, width = x.shape
    size = lax.axis_size("seq")
    cut = x.reshape(frames, size, pixels // size, width).transpose(1, 0, 2, 3)
    cut = cut.reshape(size, -1, width)
    return lax.all_to_all(cut, "seq", 0, 0, tiled=True).reshape(-1, width)


def to_frames(x, shape):
    _, frames, pixels, width = shape
    size = lax.axis_size("seq")
    back = lax.all_to_all(x.reshape(size, -1, width), "seq", 0, 0, tiled=True)
    back = back.reshape(size, frames, pixels // size, width).transpose(1, 0, 2, 3)
    return back.reshape(shape)


def block_step(latents, modulation, in_weight, out_weight, up_weight, down_weight, cotangent):
    width = latents.shape[-1]
    local = out_weight.shape[0]
    units = up_weight.shape[1]
    block = latents.shape[2] // lax.axis_size("seq")
    mod = modulation[0]
    wi = in_weight.reshape(width, 3 * local)
    tokens = to_pixels(latents)
    upstream = to_pixels(cotangent)
    n = tokens.shape[0]
    low = ((n, width), BF16)
    wide = ((n, width), F32)

    first_input = call(first_kernel, [low], tokens, mod, flops=20 * n * width)[0]
    first_full = gathered(first_input)
    branch = call(branch_kernel, [low], upstream, mod, flops=4 * n * width)[0]
    branch_full = gathered(branch)

    heads = local // HEAD_DIM
    attn_flops = 2 * n * width * 4 * local + 4 * heads * n * n * local
    projected, attended, parts = [], [], []
    for piece in first_full:
        proj, att, part = call(
            functools.partial(attend_kernel, block=block),
            [((n, 3 * local), BF16), ((n, local), BF16), low],
            piece, wi, out_weight, flops=attn_flops,
        )
        projected.append(proj)
        attended.append(att)
        parts.append(part)
    midway, second_input = call(
        midway_kernel, [wide, low], tokens, mod, *returned(parts),
        flops=20 * n * width,
    )
    second_full = gathered(second_input)
    activated, hidden_grad, parts = [], [], []
    for piece, b in zip(second_full, branch_full):
        act, hg, part = call(
            mlp_kernel,
            [((n, units), BF16), ((n, units), BF16), low],
            piece, b, up_weight, down_weight, flops=6 * n * width * units,
        )
        activated.append(act)
        hidden_grad.append(hg)
        parts.append(part)
    midway_grad, attention_grad = call(
        midgrad_kernel, [wide, low], upstream, midway, mod, *returned(parts),
        flops=30 * n * width,
    )
    torus = Torus()
    mlp_chunks = weight_grads([(branch_full, activated), (second_full, hidden_grad)], torus.order())
    mlp_sum = torus.scatter_sum(mlp_chunks)

    attention_full = gathered(attention_grad)
    projected_grad, parts = [], []
    for piece, proj in zip(attention_full, projected):
        dproj, part = call(
            functools.partial(attend_back_kernel, block=block),
            [((n, 3 * local), BF16), low],
            piece, proj, wi, out_weight, flops=2 * attn_flops,
        )
        projected_grad.append(dproj)
        parts.append(part)
    latents_grad = call(
        last_kernel, [low], tokens, midway_grad, mod, *returned(parts),
        flops=30 * n * width,
    )[0]

    ff = [
        call(product_kernel, [low], a, down_weight, flops=2 * n * width * units)[0]
        for a in activated
    ]
    result = call(result_kernel, [low], midway, mod, *returned(ff), flops=10 * n * width)[0]

    attn_chunks = weight_grads(
        [(first_full, projected_grad), (attention_full, attended)], torus.order()
    )
    attn_sum = torus.scatter_sum(attn_chunks)
    rows = width // (lax.axis_size("dp") * lax.axis_size("seq"))
    in_grad = attn_sum[:rows, : 3 * local].reshape(rows, 3, local)
    out_grad = attn_sum[:rows, 3 * local :].T
    down_grad = mlp_sum[:rows, :units].T
    up_grad = mlp_sum[:rows, units:]
    return (
        to_frames(result, latents.shape),
        to_frames(latents_grad, latents.shape),
        in_grad,
        out_grad,
        up_grad,
        down_grad,
    )


def solution(mesh):
    placed = (
        P("dp", "seq", "tensor", None),
        P("dp", None, None),
        P(None, None, "tensor"),
        P("tensor", None),
        P(None, "tensor"),
        P("tensor", None),
        P("dp", "seq", "tensor", None),
    )
    return jax.shard_map(
        block_step,
        mesh=mesh,
        in_specs=placed,
        out_specs=(
            P("dp", "seq", "tensor", None),
            P("dp", "seq", "tensor", None),
            P(("dp", "seq"), None, "tensor"),
            P("tensor", ("dp", "seq")),
            P(("dp", "seq"), "tensor"),
            P("tensor", ("dp", "seq")),
        ),
        check_vma=False,
    )
```
